128 devices in a mesh: grp: 8 (over x, z_lo), mem: 16 (over z_hi, y, core).
Axes of the slice: x: 4, y: 4, z: 4 (z_hi: 2, z_lo: 2; z = z_hi * 2 + z_lo), core: 2. Of those that a mesh axis runs over, the one named last changes fastest.
Arguments:
- weight: bfloat16 [4, 8192, 16384], P(None, None, ('grp', 'mem')), may hold values from -0.046875 to 0.046875
- activation: bfloat16 [2, 16384, 512], P(None, ('grp', 'mem')), may hold values from -6 to 6
- points: int32 [8], replicated, may hold values from 0 to 7, each once
Outputs:
- share: float32 [8, 8192, 512], P('grp', 'mem')
The draws below stay inside these ranges and needn't reach their ends.
Inputs may be any that keep to these rules, and one draw needn't show every extreme that they name: A permutation of 0 to 7; group g evaluates at points[g] + 1.
All inputs are finite; a program needn't handle non-finite values.
Results may differ from the reference program's by a relative error of at most 0.0042.
Values may be sent and summed in bfloat16 or wider, within the bound.
A program may use at most 320 MiB of HBM per device.

```python
import jax
import jax.numpy as jnp

D = 16384
C = 512
SPLITS = 2
BLOCKS = 4
FB = 8192
N_GRP = 8


def steps_of(own_key, extent, cuts, low, high):
    level = 1.0
    for dim, blocks in cuts:
        steps = jax.random.uniform(jax.random.fold_in(jax.random.fold_in(own_key, 6), dim), (blocks,), jnp.float32, low / len(cuts), high / len(cuts))
        level = level * jnp.repeat(jnp.exp(steps), extent[dim] // blocks).reshape((-1,) + (1,) * (len(extent) - 1 - dim))
    return level


def scatter_about(stream_key, dims, width, bound, cuts=(), held_as=jnp.bfloat16):
    entries = width * jax.random.normal(stream_key, dims, jnp.float32)
    if cuts:
        entries = entries * steps_of(stream_key, dims, cuts, -0.22, 0.18)
    return jnp.clip(entries, -bound, bound).astype(held_as)


def setup_inputs(seed: int = 0) -> dict:
    keys = jax.random.split(jax.random.key(seed), 4)
    weight = scatter_about(keys[0], (BLOCKS, FB, D), D ** -0.5, 0.046875, ((2, 128),))
    activation = scatter_about(keys[1], (SPLITS, D, C), 1.0, 6.0, ((1, 128),))
    points = jax.random.permutation(keys[2], N_GRP).astype(jnp.int32)
    return {"weight": weight, "activation": activation, "points": points}


def reference(weight, activation, points):
    anchors = (points + 1).astype(jnp.float32) / N_GRP
    weight_powers = jnp.arange(BLOCKS, dtype=jnp.float32)
    input_powers = jnp.arange(SPLITS, dtype=jnp.float32) * BLOCKS
    shares = []
    for group in range(N_GRP):
        factors = anchors[group] ** weight_powers
        total = factors[0] * weight[0].astype(jnp.float32)
        for block in range(1, BLOCKS):
            total = total + factors[block] * weight[block].astype(jnp.float32)
        coded_weight = total.astype(jnp.bfloat16)
        lifts = anchors[group] ** input_powers
        mixed = lifts[0] * activation[0].astype(jnp.float32)
        for split in range(1, SPLITS):
            mixed = mixed + lifts[split] * activation[split].astype(jnp.float32)
        coded_input = mixed.astype(jnp.bfloat16)
        shares.append(jnp.dot(coded_weight, coded_input, preferred_element_type=jnp.float32))
    return jnp.stack(shares)
```

```python
import functools

import jax
import jax.numpy as jnp
from jax import lax
from jax.experimental import pallas as pl
from jax.experimental.pallas import tpu as pltpu
from jax.sharding import PartitionSpec as P

MESH = pl.DeviceIdType.MESH
ROWS = 512
WIDTH = 32
STEPS = ROWS // WIDTH
AHEAD = 3
LAG = 2


def place():
    grp, mem = lax.axis_index("grp"), lax.axis_index("mem")
    return grp // 2, (mem // 2) % 4, (mem // 8) * 2 + grp % 2, mem % 2


def device(x, y, z, core):
    return (x * 2 + z % 2, (z // 2) * 8 + y * 2 + core)


def kernel(weight, act, points, out, slab, feats, prods, sent, got, total,
           slab_sem, slab_out, feat_sem, feat_out, got_sem, got_out, own_sem, out_sem):
    x, y, z, core = place()
    line = [(dy, dc) for dy in (2, 1, 3, 0) for dc in (0, 1) if dy or dc]
    plane = [(dx, dz) for dx in (2, 1, 3, 0) for dz in (2, 1, 3, 0) if dx or dz]
    mine = y * 2 + core
    spot = x * 4 + z

    def line_peer(dy, dc):
        return lax.rem(y + dy, 4), lax.rem(core + dc, 2)

    def plane_peer(dx, dz):
        return lax.rem(x + dx, 4), lax.rem(z + dz, 4)

    barrier = pltpu.get_barrier_semaphore()
    for dy, dc in line:
        py, pc = line_peer(dy, dc)
        pl.semaphore_signal(barrier, inc=1, device_id=device(x, py, z, pc), device_id_type=MESH)
    for dx, dz in plane:
        px, pz = plane_peer(dx, dz)
        pl.semaphore_signal(barrier, inc=1, device_id=device(px, y, pz, core), device_id_type=MESH)
    pl.semaphore_wait(barrier, len(line) + len(plane))

    def lanes(index):
        return pl.ds(pl.multiple_of(index * 128, 128), 128)

    def feat_slot(index):
        return feats.at[:, lanes(index), :]

    def feat_copy(source, index, py, pc, order):
        return pltpu.make_async_remote_copy(
            src_ref=source, dst_ref=feat_slot(index), send_sem=feat_out.at[order],
            recv_sem=feat_sem.at[index], device_id=device(x, py, z, pc), device_id_type=MESH)

    def slab_copy(step, dy, dc):
        py, pc = line_peer(dy, dc)
        start = pl.multiple_of((py * 2 + pc) * ROWS + step * WIDTH, WIDTH)
        return pltpu.make_async_remote_copy(
            src_ref=weight.at[:, :, pl.ds(start, WIDTH), :],
            dst_ref=slab.at[step, :, :, :, lanes(mine)],
            send_sem=slab_out.at[step, dy * 2 + dc], recv_sem=slab_sem.at[step, mine],
            device_id=device(x, py, z, pc), device_id_type=MESH)

    def slab_own(step):
        start = pl.multiple_of(mine * ROWS + step * WIDTH, WIDTH)
        return pltpu.make_async_copy(
            weight.at[:, :, pl.ds(start, WIDTH), :], slab.at[step, :, :, :, lanes(mine)], own_sem.at[step])

    def slab_arrival(step, dy, dc):
        py, pc = line_peer(dy, dc)
        index = py * 2 + pc
        return pltpu.make_async_remote_copy(
            src_ref=weight.at[:, :, pl.ds(0, WIDTH), :],
            dst_ref=slab.at[step, :, :, :, lanes(index)],
            send_sem=slab_out.at[step, dy * 2 + dc], recv_sem=slab_sem.at[step, index],
            device_id=device(x, py, z, pc), device_id_type=MESH)

    def share_copy(step, dx, dz):
        px, pz = plane_peer(dx, dz)
        return pltpu.make_async_remote_copy(
            src_ref=sent.at[step, px * 4 + pz], dst_ref=got.at[step, spot],
            send_sem=got_out.at[step, dx * 4 + dz], recv_sem=got_sem.at[step, spot],
            device_id=device(px, y, pz, core), device_id_type=MESH)

    def share_arrival(step, dx, dz):
        px, pz = plane_peer(dx, dz)
        index = px * 4 + pz
        return pltpu.make_async_remote_copy(
            src_ref=sent.at[step, index], dst_ref=got.at[step, index],
            send_sem=got_out.at[step, dx * 4 + dz], recv_sem=got_sem.at[step, index],
            device_id=device(px, y, pz, core), device_id_type=MESH)

    def send_slab(step):
        slab_own(step).start()
        for dy, dc in line:
            slab_copy(step, dy, dc).start()

    own_feat = pltpu.make_async_copy(act, feat_slot(mine), out_sem.at[STEPS])
    own_feat.start()
    for order, (dy, dc) in enumerate(((2, 0), (1, 0), (3, 0), (0, 1))):
        py, pc = line_peer(dy, dc)
        feat_copy(act, mine, py, pc, order).start()
    for step in range(AHEAD):
        send_slab(step)
    for order, dy in enumerate((1, 3, 2)):
        py = lax.rem(y + dy, 4)
        index = py * 2 + core
        feat_copy(act, index, py, core, order).wait_recv()
        feat_copy(feat_slot(index), index, y, 1 - core, 4 + order).start()
    own_feat.wait()
    for dy in range(4):
        py = lax.rem(y + dy, 4)
        feat_copy(act, py * 2 + 1 - core, y, 1 - core, 3).wait_recv()

    anchors = [(points[g] + 1).astype(jnp.float32) * 0.125 for g in range(8)]

    def out_copy(step):
        rows = pl.ds(pl.multiple_of(step * WIDTH, WIDTH), WIDTH)
        return pltpu.make_async_copy(total.at[rows], out.at[0, rows], out_sem.at[step])

    def finish(step):
        for dx, dz in plane:
            share_arrival(step, dx, dz).wait_recv()

        def add(tile, carry):
            rows = pl.ds(pl.multiple_of(tile * 16, 16), 16)
            value = sent[step, spot, rows, :].astype(jnp.float32)
            for dx, dz in plane:
                px, pz = plane_peer(dx, dz)
                value = value + got[step, px * 4 + pz, rows, :].astype(jnp.float32)
            total[pl.ds(pl.multiple_of(step * WIDTH + tile * 16, 16), 16), :] = value
            return carry

        lax.fori_loop(0, WIDTH // 16, add, 0)
        out_copy(step).start()

    def body(step, carry):
        @pl.when(step + AHEAD < STEPS)
        def _():
            send_slab(step + AHEAD)

        slab_own(step).wait()
        for dy, dc in line:
            slab_arrival(step, dy, dc).wait_recv()
        left = slab[step].reshape(8 * WIDTH, 1024)
        for k in range(2):
            prods[k] = jnp.dot(left, feats[k], preferred_element_type=jnp.float32).reshape(4, 2, WIDTH, 512)

        def combine(tile, carry):
            half = tile // (WIDTH // 16)
            rows = pl.ds(pl.multiple_of((tile % (WIDTH // 16)) * 16, 16), 16)
            for part in range(2):
                cols = pl.ds(part * 256, 256)
                terms = [prods[p // 4, p % 4, half, rows, cols] for p in range(8)]
                for g in range(8):
                    value = terms[7]
                    for p in range(6, -1, -1):
                        value = value * anchors[g] + terms[p]
                    sent[step, (g // 2) * 4 + half * 2 + g % 2, rows, cols] = value.astype(jnp.bfloat16)
            return carry

        lax.fori_loop(0, 2 * WIDTH // 16, combine, 0)
        for dx, dz in plane:
            share_copy(step, dx, dz).start()

        @pl.when(step >= LAG)
        def _():
            finish(step - LAG)

        return carry

    lax.fori_loop(0, STEPS, body, 0)
    lax.fori_loop(STEPS - LAG, STEPS, lambda step, c: (finish(step), c)[1], 0)

    for order, (dy, dc) in enumerate(((2, 0), (1, 0), (3, 0), (0, 1))):
        py, pc = line_peer(dy, dc)
        feat_copy(act, mine, py, pc, order).wait_send()
    for order, dy in enumerate((1, 3, 2)):
        index = lax.rem(y + dy, 4) * 2 + core
        feat_copy(feat_slot(index), index, y, 1 - core, 4 + order).wait_send()

    def drain(step, carry):
        for dy, dc in line:
            slab_copy(step, dy, dc).wait_send()
        for dx, dz in plane:
            share_copy(step, dx, dz).wait_send()
        out_copy(step).wait()
        return carry

    lax.fori_loop(0, STEPS, drain, 0)


def per_device(weight, activation, points):
    any_space = pl.BlockSpec(memory_space=pl.ANY)
    dma = pltpu.SemaphoreType.DMA
    return pl.pallas_call(
        kernel,
        out_shape=jax.ShapeDtypeStruct((1, ROWS, 512), jnp.float32),
        in_specs=[any_space, any_space, pl.BlockSpec(memory_space=pltpu.SMEM)],
        out_specs=any_space,
        scratch_shapes=[
            pltpu.VMEM((STEPS, 4, 2, WIDTH, 1024), jnp.bfloat16),
            pltpu.VMEM((2, 1024, 512), jnp.bfloat16),
            pltpu.VMEM((2, 4, 2, WIDTH, 512), jnp.float32),
            pltpu.VMEM((STEPS, 16, WIDTH, 512), jnp.bfloat16),
            pltpu.VMEM((STEPS, 16, WIDTH, 512), jnp.bfloat16),
            pltpu.VMEM((ROWS, 512), jnp.float32),
            dma((STEPS, 8)), dma((STEPS, 8)), dma((8,)), dma((7,)),
            dma((STEPS, 16)), dma((STEPS, 16)), dma((STEPS,)), dma((STEPS + 1,)),
        ],
        compiler_params=pltpu.CompilerParams(
            collective_id=0, has_side_effects=True, vmem_limit_bytes=48 * 2**20),
        name="coded_share",
    )(weight.reshape(4, 2, 4096, 128), activation, points)


def solution(mesh):
    placed = (P(None, None, ("grp", "mem")), P(None, ("grp", "mem"), None), P())
    return jax.shard_map(
        per_device, mesh=mesh, in_specs=placed, out_specs=P("grp", "mem", None), check_vma=False
    )
```

```python
import jax
import jax.numpy as jnp
from jax import lax
from jax.experimental import pallas as pl
from jax.experimental.pallas import tpu as pltpu
from jax.sharding import PartitionSpec as P

MESH = pl.DeviceIdType.MESH
STEPS = 8
WA = 32
WB = 16
BASE_B = STEPS * WA
AHEAD = 2
OTHER_A = (2, 5)
OTHER_B = (1, 4, 6)
LAG1 = 3
LAG2 = 6


def place():
    grp, mem = lax.axis_index("grp"), lax.axis_index("mem")
    return grp // 2, (mem // 2) % 4, (mem // 8) * 2 + grp % 2, mem % 2


def device(x, y, z, core):
    return (x * 2 + z % 2, (z // 2) * 8 + y * 2 + core)


def kernel(weight, act, points, out, slab_a, slab_b, feats, prods, part, part_in, sums, sums_in, anchor_mem,
           slab_sem, slab_out, own_sem, feat_sem, feat_out, one_sem, two_sem, one_out, two_out, misc_sem):
    x, y, z, core = place()
    low = z % 2
    gather_order = [(d, e) for d in (2, 1, 3, 0) for e in (0, 1) if d or e]
    swap_order = [(d, e) for d in (2, 1, 3, 0) for e in (0, 1) if d or e]

    def at(xx, yy, zz, cc):
        return device(lax.rem(xx, 4), lax.rem(yy, 4), lax.rem(zz, 4), lax.rem(cc, 2))

    def swapped(e):
        return (z // 2) * 2 + lax.rem(low + e, 2)

    peers = [at(x, y + d, z, core + e) for d in range(4) for e in range(2) if d or e]
    peers += [at(x, y, z + d, core + e) for d in range(1, 4) for e in range(2)]
    peers += [at(x + d, y, z, core) for d in range(1, 4)]
    peers += [at(x, y + d, swapped(1), core) for d in range(1, 4)]
    peers += [at(x + d, y, swapped(1), core) for d in range(1, 4)]
    barrier = pltpu.get_barrier_semaphore()
    for peer in peers:
        pl.semaphore_signal(barrier, inc=1, device_id=peer, device_id_type=MESH)
    pl.semaphore_wait(barrier, len(peers))

    def lanes(index):
        return pl.ds(pl.multiple_of(index * 128, 128), 128)

    def line_at(kind, d, e):
        return at(x, y + d, z, core + e) if kind == 0 else at(x, y, z + d, core + e)

    def line_pos(kind):
        return y if kind == 0 else z

    def line_index(kind, d, e):
        return lax.rem(line_pos(kind) + d, 4) * 2 + lax.rem(core + e, 2)

    def feat_slot(kind, index):
        return feats.at[kind, :, lanes(index), :]

    def feat_copy(kind, source, index, d, e, order):
        return pltpu.make_async_remote_copy(
            src_ref=source, dst_ref=feat_slot(kind, index), send_sem=feat_out.at[kind, order],
            recv_sem=feat_sem.at[kind, index], device_id=line_at(kind, d, e), device_id_type=MESH)

    def rows_for(kind, step, d, e):
        pos, cc = lax.rem(line_pos(kind) + d, 4), lax.rem(core + e, 2)
        if kind == 0:
            start = pl.multiple_of(step * WA, WA)
            return weight.at[:, :, pos, cc, pl.ds(start, WA), :]
        start = pl.multiple_of(BASE_B + (pos % 2) * (STEPS * WB) + step * WB, WB)
        return weight.at[:, pos // 2, :, cc, pl.ds(start, WB), :]

    def slab_slot(kind, step, index):
        slab = slab_a if kind == 0 else slab_b
        return slab.at[step, :, :, :, lanes(index)]

    def slab_copy(kind, step, d, e):
        mine = line_index(kind, 0, 0)
        return pltpu.make_async_remote_copy(
            src_ref=rows_for(kind, step, d, e), dst_ref=slab_slot(kind, step, mine),
            send_sem=slab_out.at[kind, step, d * 2 + e], recv_sem=slab_sem.at[kind, step, mine],
            device_id=line_at(kind, d, e), device_id_type=MESH)

    def slab_arrival(kind, step, d, e):
        index = line_index(kind, d, e)
        return pltpu.make_async_remote_copy(
            src_ref=rows_for(kind, step, d, e), dst_ref=slab_slot(kind, step, index),
            send_sem=slab_out.at[kind, step, d * 2 + e], recv_sem=slab_sem.at[kind, step, index],
            device_id=line_at(kind, d, e), device_id_type=MESH)

    def slab_own(kind, step):
        return pltpu.make_async_copy(
            rows_for(kind, step, 0, 0), slab_slot(kind, step, line_index(kind, 0, 0)), own_sem.at[kind, step])

    def send_slab(kind, step):
        slab_own(kind, step).start()
        for d, e in gather_order:
            slab_copy(kind, step, d, e).start()

    def first_axis(kind, step):
        other = OTHER_A if kind == 0 else OTHER_B
        flag = jnp.int32(1)
        for k in other:
            flag = flag - (step == k).astype(jnp.int32)
        return flag

    def one_pos(kind, f):
        return f * x + (1 - f) * (z if kind == 0 else y)

    def one_at(kind, f, d):
        if kind == 0:
            return at(x + f * d, y, z + (1 - f) * d, core)
        return at(x + f * d, y + (1 - f) * d, z, core)

    def one_copy(kind, step, d):
        f = first_axis(kind, step)
        mine = one_pos(kind, f)
        return pltpu.make_async_remote_copy(
            src_ref=part.at[kind, step, lax.rem(mine + d, 4)], dst_ref=part_in.at[kind, step, mine],
            send_sem=one_out.at[kind, step, d], recv_sem=one_sem.at[kind, step, mine],
            device_id=one_at(kind, f, d), device_id_type=MESH)

    def one_arrival(kind, step, d):
        f = first_axis(kind, step)
        index = lax.rem(one_pos(kind, f) + d, 4)
        return pltpu.make_async_remote_copy(
            src_ref=part.at[kind, step, index], dst_ref=part_in.at[kind, step, index],
            send_sem=one_out.at[kind, step, d], recv_sem=one_sem.at[kind, step, index],
            device_id=one_at(kind, f, d), device_id_type=MESH)

    def two_pos(kind, f):
        return f * (z if kind == 0 else y) + (1 - f) * x

    def two_at(kind, f, d, e):
        if kind == 0:
            return at(x + (1 - f) * d, y, z + f * d, core)
        return at(x + (1 - f) * d, y + f * d, swapped(e), core)

    def two_rows(kind, f, d, e):
        pos = lax.rem(two_pos(kind, f) + d, 4)
        if kind == 0:
            return pl.ds(pl.multiple_of(pos * WA, WA), WA)
        zl = lax.rem(low + e, 2)
        sub = f * (zl * 4 + pos) + (1 - f) * (pos * 2 + zl)
        return pl.ds(pl.multiple_of(sub * WB, WB), WB)

    def two_slot(kind, f, d, e):
        pos = lax.rem(two_pos(kind, f) + d, 4)
        return pos if kind == 0 else pos * 2 + lax.rem(low + e, 2)

    def slot_rows(kind, slot):
        width = WA if kind == 0 else WB
        return pl.ds(pl.multiple_of(slot * width, width), width)

    def two_list(kind):
        return [(2, 0), (1, 0), (3, 0)] if kind == 0 else swap_order

    def two_copy(kind, step, d, e):
        f = first_axis(kind, step)
        mine = two_slot(kind, f, 0, 0)
        return pltpu.make_async_remote_copy(
            src_ref=sums.at[kind, step, two_rows(kind, f, d, e), :],
            dst_ref=sums_in.at[kind, step, slot_rows(kind, mine), :],
            send_sem=two_out.at[kind, step, d * 2 + e], recv_sem=two_sem.at[kind, step, mine],
            device_id=two_at(kind, f, d, e), device_id_type=MESH)

    def two_arrival(kind, step, d, e):
        f = first_axis(kind, step)
        slot = two_slot(kind, f, d, e)
        return pltpu.make_async_remote_copy(
            src_ref=sums.at[kind, step, two_rows(kind, f, d, e), :],
            dst_ref=sums_in.at[kind, step, slot_rows(kind, slot), :],
            send_sem=two_out.at[kind, step, d * 2 + e], recv_sem=two_sem.at[kind, step, slot],
            device_id=two_at(kind, f, d, e), device_id_type=MESH)

    points_copy = pltpu.make_async_copy(points, anchor_mem, misc_sem.at[0])
    points_copy.start()
    feat_order = [(2, 0), (1, 0), (3, 0), (0, 1)]
    own_feats = [pltpu.make_async_copy(act, feat_slot(kind, line_index(kind, 0, 0)), misc_sem.at[1 + kind]) for kind in range(2)]
    for order, (d, e) in enumerate(feat_order):
        for kind in range(2):
            feat_copy(kind, act, line_index(kind, 0, 0), d, e, order).start()
    for copy in own_feats:
        copy.start()
    for step in range(AHEAD):
        for kind in range(2):
            send_slab(kind, step)
    for order, d in enumerate((1, 3, 2)):
        for kind in range(2):
            index = line_index(kind, d, 0)
            feat_copy(kind, act, index, d, 0, order).wait_recv()
            feat_copy(kind, feat_slot(kind, index), index, 0, 1, 4 + order).start()
    points_copy.wait()
    for kind in range(2):
        own_feats[kind].wait()
        for d in range(4):
            feat_copy(kind, act, line_index(kind, d, 1), 0, 1, 3).wait_recv()

    anchors = [(anchor_mem[g] + 1).astype(jnp.float32) * 0.125 for g in range(8)]

    def produce(kind, step):
        f = first_axis(kind, step)
        slab_own(kind, step).wait()
        for d, e in gather_order:
            slab_arrival(kind, step, d, e).wait_recv()
        slab = slab_a if kind == 0 else slab_b
        left = slab[step].reshape(256, 1024)
        for k in range(2):
            prods[k] = jnp.dot(left, feats[kind, k], preferred_element_type=jnp.float32).reshape(4, 64, 512)

        def combine(tile, carry):
            rows = pl.ds(pl.multiple_of(tile * 16, 16), 16)
            for half in range(2):
                cols = pl.ds(half * 256, 256)
                terms = [prods[p // 4, p % 4, rows, cols] for p in range(8)]
                for g in range(8):
                    value = terms[7]
                    for p in range(6, -1, -1):
                        value = value * anchors[g] + terms[p]
                    gx, zl = g // 2, g % 2
                    if kind == 0:
                        zz, inner = (tile // 2) * 2 + zl, (tile % 2) * 16
                        owner = f * gx + (1 - f) * zz
                        row = (f * zz + (1 - f) * gx) * WA + inner
                    else:
                        owner = f * gx + (1 - f) * tile
                        row = (f * (zl * 4 + tile) + (1 - f) * (gx * 2 + zl)) * WB
                    part[kind, step, owner, pl.ds(pl.multiple_of(row, 16), 16), cols] = value.astype(jnp.bfloat16)
            return carry

        lax.fori_loop(0, 4, combine, 0)
        for d in (2, 1, 3):
            one_copy(kind, step, d).start()

    def middle(kind, step):
        f = first_axis(kind, step)
        for d in range(1, 4):
            one_arrival(kind, step, d).wait_recv()
        mine = one_pos(kind, f)

        def add(tile, carry):
            rows = pl.ds(pl.multiple_of(tile * 16, 16), 16)
            value = part[kind, step, mine, rows, :].astype(jnp.float32)
            for d in range(1, 4):
                value = value + part_in[kind, step, lax.rem(mine + d, 4), rows, :].astype(jnp.float32)
            sums[kind, step, rows, :] = value.astype(jnp.bfloat16)
            return carry

        lax.fori_loop(0, 8, add, 0)
        for d, e in two_list(kind):
            two_copy(kind, step, d, e).start()

    def last(kind, step):
        f = first_axis(kind, step)
        for d, e in two_list(kind):
            two_arrival(kind, step, d, e).wait_recv()
        own = sums[kind, step, two_rows(kind, f, 0, 0), :].astype(jnp.float32)
        if kind == 0:
            value = own
            for d in range(1, 4):
                value = value + sums_in[kind, step, slot_rows(kind, two_slot(kind, f, d, 0)), :].astype(jnp.float32)
            out[0, pl.ds(pl.multiple_of(step * WA, WA), WA), :] = value
        else:
            for e in range(2):
                value = own if e == 0 else None
                for d in range(4):
                    if d or e:
                        piece = sums_in[kind, step, slot_rows(kind, two_slot(kind, f, d, e)), :].astype(jnp.float32)
                        value = piece if value is None else value + piece
                row = BASE_B + lax.rem(low + e, 2) * (STEPS * WB) + step * WB
                out[0, pl.ds(pl.multiple_of(row, WB), WB), :] = value

    def body(step, carry):
        @pl.when(step + AHEAD < STEPS)
        def _():
            for kind in range(2):
                send_slab(kind, step + AHEAD)

        for kind in range(2):
            produce(kind, step)

            @pl.when(step >= LAG1)
            def _():
                middle(kind, step - LAG1)

        @pl.when(step >= LAG2)
        def _():
            for kind in range(2):
                last(kind, step - LAG2)

        return carry

    lax.fori_loop(0, STEPS, body, 0)
    def finish(step, carry):
        @pl.when(step < STEPS + LAG1)
        def _():
            for kind in range(2):
                middle(kind, step - LAG1)

        for kind in range(2):
            last(kind, step - LAG2)
        return carry

    lax.fori_loop(STEPS, STEPS + LAG2, finish, 0)

    for kind in range(2):
        for order, (d, e) in enumerate(feat_order):
            feat_copy(kind, act, line_index(kind, 0, 0), d, e, order).wait_send()
        for order, d in enumerate((1, 3, 2)):
            index = line_index(kind, d, 0)
            feat_copy(kind, feat_slot(kind, index), index, 0, 1, 4 + order).wait_send()

    def drain(step, carry):
        for kind in range(2):
            for d, e in gather_order:
                slab_copy(kind, step, d, e).wait_send()
            for d in range(1, 4):
                one_copy(kind, step, d).wait_send()
            for d, e in two_list(kind):
                two_copy(kind, step, d, e).wait_send()
        return carry

    lax.fori_loop(0, STEPS, drain, 0)


def per_device(weight, activation, points):
    hbm = pl.BlockSpec(memory_space=pltpu.HBM)
    dma = pltpu.SemaphoreType.DMA
    return pl.pallas_call(
        kernel,
        out_shape=jax.ShapeDtypeStruct((1, 512, 512), jnp.float32),
        in_specs=[hbm, hbm, hbm],
        out_specs=pl.BlockSpec(memory_space=pltpu.VMEM),
        scratch_shapes=[
            pltpu.VMEM((STEPS, 4, 2, WA, 1024), jnp.bfloat16),
            pltpu.VMEM((STEPS, 4, 4, WB, 1024), jnp.bfloat16),
            pltpu.VMEM((2, 2, 1024, 512), jnp.bfloat16),
            pltpu.VMEM((2, 4, 64, 512), jnp.float32),
            pltpu.VMEM((2, STEPS, 4, 128, 512), jnp.bfloat16),
            pltpu.VMEM((2, STEPS, 4, 128, 512), jnp.bfloat16),
            pltpu.VMEM((2, STEPS, 128, 512), jnp.bfloat16),
            pltpu.VMEM((2, STEPS, 128, 512), jnp.bfloat16),
            pltpu.SMEM((8,), jnp.int32),
            dma((2, STEPS, 8)), dma((2, STEPS, 8)), dma((2, STEPS)), dma((2, 8)), dma((2, 7)),
            dma((2, STEPS, 4)), dma((2, STEPS, 8)), dma((2, STEPS, 4)), dma((2, STEPS, 8)), dma((3,)),
        ],
        compiler_params=pltpu.CompilerParams(
            collective_id=0, has_side_effects=True, vmem_limit_bytes=52 * 2**20),
        name="coded_share",
    )(weight.reshape(4, 2, 4, 2, 512, 128), activation, points)


def solution(mesh):
    placed = (P(None, None, ("grp", "mem")), P(None, ("grp", "mem"), None), P())
    return jax.shard_map(
        per_device, mesh=mesh, in_specs=placed, out_specs=P("grp", "mem", None), check_vma=False
    )
```

```python
import jax
import jax.numpy as jnp
from jax import lax
from jax.experimental import pallas as pl
from jax.experimental.pallas import tpu as pltpu
from jax.sharding import PartitionSpec as P

MESH = pl.DeviceIdType.MESH
STEPS = 8
WA = 32
WB = 16
BASE_B = STEPS * WA
AHEAD = 8
OTHER_A = (5, 6)
OTHER_B = (5, 6)
LAG0 = 2
LAG1 = 4
LAG2 = 8


def place():
    grp, mem = lax.axis_index("grp"), lax.axis_index("mem")
    return grp // 2, (mem // 2) % 4, (mem // 8) * 2 + grp % 2, mem % 2


def device(x, y, z, core):
    return (x * 2 + z % 2, (z // 2) * 8 + y * 2 + core)


def kernel(weight, act, points, out, slab_a, slab_b, feats, prods, part, relay, part_in, sums, sums_in, swap, anchor_mem,
           slab_sem, slab_out, feat_sem, pair_sem, feat_out, one_sem, one_out, two_sem, two_out, swap_sem, swap_out,
           misc_sem):
    x, y, z, core = place()
    low = z % 2
    gather_order = [(d, e) for d in (2, 1, 3, 0) for e in (0, 1) if d or e]

    def at(xx, yy, zz, cc):
        return device(lax.rem(xx, 4), lax.rem(yy, 4), lax.rem(zz, 4), lax.rem(cc, 2))

    peers = [at(x, y + d, z, core + e) for d in range(4) for e in range(2) if d or e]
    peers += [at(x, y, z + d, core + e) for d in range(1, 4) for e in range(2)]
    peers += [at(x + d, y, z, core) for d in range(1, 4)]
    barrier = pltpu.get_barrier_semaphore()
    for peer in peers:
        pl.semaphore_signal(barrier, inc=1, device_id=peer, device_id_type=MESH)
    pl.semaphore_wait(barrier, len(peers))

    def wait_for(ref, sem):
        pltpu.make_async_copy(ref, ref, sem).wait()

    def lanes(index):
        return pl.ds(pl.multiple_of(index * 128, 128), 128)

    def line_at(kind, d, e):
        return at(x, y + d, z, core + e) if kind == 0 else at(x, y, z + d, core + e)

    def line_pos(kind):
        return y if kind == 0 else z

    def line_index(kind, d, e):
        return lax.rem(line_pos(kind) + d, 4) * 2 + lax.rem(core + e, 2)

    def feat_slot(kind, index):
        return feats.at[kind, :, lanes(index), :]

    def feat_send(kind, d):
        return pltpu.make_async_remote_copy(
            src_ref=act, dst_ref=feat_slot(kind, line_index(kind, 0, 0)), send_sem=feat_out.at[kind],
            recv_sem=feat_sem.at[kind, d - 1], device_id=line_at(kind, d, 0), device_id_type=MESH)

    def feat_pair(kind, d):
        index = line_index(kind, d, 0)
        return pltpu.make_async_remote_copy(
            src_ref=act if d == 0 else feat_slot(kind, index), dst_ref=feat_slot(kind, index),
            send_sem=feat_out.at[kind], recv_sem=pair_sem.at[kind], device_id=line_at(kind, 0, 1), device_id_type=MESH)

    def rows_for(kind, step, d, e):
        pos, cc = lax.rem(line_pos(kind) + d, 4), lax.rem(core + e, 2)
        if kind == 0:
            start = pl.multiple_of(step * WA, WA)
            return weight.at[:, :, pos, cc, pl.ds(start, WA), :]
        start = pl.multiple_of(BASE_B + (pos % 2) * (STEPS * WB) + step * WB, WB)
        return weight.at[:, pos // 2, :, cc, pl.ds(start, WB), :]

    def slab_slot(kind, step, index):
        slab = slab_a if kind == 0 else slab_b
        return slab.at[step, :, :, :, lanes(index)]

    def slab_copy(kind, step, d, e):
        mine = line_index(kind, 0, 0)
        return pltpu.make_async_remote_copy(
            src_ref=rows_for(kind, step, d, e), dst_ref=slab_slot(kind, step, mine),
            send_sem=slab_out.at[kind], recv_sem=slab_sem.at[kind, step],
            device_id=line_at(kind, d, e), device_id_type=MESH)

    def slab_own(kind, step):
        return pltpu.make_async_copy(
            rows_for(kind, step, 0, 0), slab_slot(kind, step, line_index(kind, 0, 0)), slab_sem.at[kind, step])

    def send_slab(kind, step):
        slab_own(kind, step).start()
        for d, e in gather_order:
            slab_copy(kind, step, d, e).start()

    def first_axis(kind, step):
        other = OTHER_A if kind == 0 else OTHER_B
        flag = jnp.int32(1)
        for k in other:
            flag = flag - (step == k).astype(jnp.int32)
        return flag

    def one_pos(kind, f):
        return f * x + (1 - f) * (z if kind == 0 else y)

    def one_at(kind, f, d):
        if kind == 0:
            return at(x + f * d, y, z + (1 - f) * d, core)
        return at(x + f * d, y + (1 - f) * d, z, core)

    def hop(kind, step, order):
        f = first_axis(kind, step)
        mine = one_pos(kind, f)
        piece, half, way = ((2, 0, 1), (2, 1, 3), (1, 1, 1), (3, 0, 3), (1, 0, 1), (3, 1, 3))[order]
        rows = pl.ds(half * 64, 64)
        side = 0 if way == 1 else 1
        group = 0 if order < 2 else 1
        target = relay.at[kind, step, half] if order < 2 else part_in.at[kind, step, side, rows, :]
        return pltpu.make_async_remote_copy(
            src_ref=part.at[kind, step, lax.rem(mine + piece, 4), rows, :], dst_ref=target,
            send_sem=one_out.at[group], recv_sem=one_sem.at[kind, step, group],
            device_id=one_at(kind, f, way), device_id_type=MESH)

    def two_pos(kind, f):
        return f * (z if kind == 0 else y) + (1 - f) * x

    def two_at(kind, f, d):
        if kind == 0:
            return at(x + (1 - f) * d, y, z + f * d, core)
        return at(x + (1 - f) * d, y + f * d, z, core)

    def quarter(pos):
        return pl.ds(pl.multiple_of(lax.rem(pos, 4) * 32, 32), 32)

    def two_copy(kind, step, d):
        f = first_axis(kind, step)
        mine = two_pos(kind, f)
        return pltpu.make_async_remote_copy(
            src_ref=sums.at[kind, step, quarter(mine + d), :], dst_ref=sums_in.at[kind, step, quarter(mine), :],
            send_sem=two_out.at[0], recv_sem=two_sem.at[kind, step],
            device_id=two_at(kind, f, d), device_id_type=MESH)

    def row_b(which, step):
        return pl.ds(pl.multiple_of(BASE_B + which * (STEPS * WB) + step * WB, WB), WB)

    def swap_copy(step, which):
        rows = row_b(which, step)
        return pltpu.make_async_remote_copy(
            src_ref=swap.at[step], dst_ref=out.at[0, rows, :], send_sem=swap_out.at[0], recv_sem=swap_sem.at[0],
            device_id=at(x, y, (z // 2) * 2 + 1 - low, core), device_id_type=MESH)

    points_copy = pltpu.make_async_copy(points, anchor_mem, misc_sem.at[0])
    points_copy.start()
    own_feats = [pltpu.make_async_copy(act, feat_slot(kind, line_index(kind, 0, 0)), misc_sem.at[1 + kind]) for kind in range(2)]
    for d in (2, 1, 3):
        for kind in range(2):
            feat_send(kind, d).start()
    for kind in range(2):
        own_feats[kind].start()
        feat_pair(kind, 0).start()
    for step in range(AHEAD):
        for kind in range(2):
            send_slab(kind, step)
    for d in (1, 3, 2):
        for kind in range(2):
            wait_for(feat_slot(kind, line_index(kind, d, 0)), feat_sem.at[kind, 3 - d])
            feat_pair(kind, d).start()
    points_copy.wait()
    for kind in range(2):
        own_feats[kind].wait()
        wait_for(feats.at[kind, :, pl.ds(0, 512), :], pair_sem.at[kind])

    anchors = [(anchor_mem[g] + 1).astype(jnp.float32) * 0.125 for g in range(8)]

    def produce(kind, step):
        f = first_axis(kind, step)
        slab = slab_a if kind == 0 else slab_b
        wait_for(slab.at[step], slab_sem.at[kind, step])
        left = slab[step].reshape(256, 1024)
        for k in range(2):
            prods[k] = jnp.dot(left, feats[kind, k], preferred_element_type=jnp.float32).reshape(4, 64, 512)

        def combine(tile, carry):
            rows = pl.ds(pl.multiple_of(tile * 16, 16), 16)
            for half in range(2):
                cols = pl.ds(half * 256, 256)
                terms = [prods[p // 4, p % 4, rows, cols] for p in range(8)]
                for g in range(8):
                    value = terms[7]
                    for p in range(6, -1, -1):
                        value = value * anchors[g] + terms[p]
                    gx, zl = g // 2, g % 2
                    if kind == 0:
                        zz, inner = (tile // 2) * 2 + zl, (tile % 2) * 16
                        owner = f * gx + (1 - f) * zz
                        row = (f * zz + (1 - f) * gx) * WA + inner
                    else:
                        owner = f * gx + (1 - f) * tile
                        row = (f * tile + (1 - f) * gx) * 32 + zl * WB
                    part[kind, step, owner, pl.ds(pl.multiple_of(row, 16), 16), cols] = value.astype(jnp.bfloat16)
            return carry

        lax.fori_loop(0, 4, combine, 0)
        for order in range(4):
            hop(kind, step, order).start()

    def forward(kind, step):
        f = first_axis(kind, step)
        mine = one_pos(kind, f)
        wait_for(relay.at[kind, step], one_sem.at[kind, step, 0])
        for half in range(2):
            piece = lax.rem(mine + (1 if half == 0 else 3), 4)

            def add(tile, carry):
                rows = pl.ds(pl.multiple_of(tile * 16, 16), 16)
                where = pl.ds(pl.multiple_of(half * 64 + tile * 16, 16), 16)
                value = part[kind, step, piece, where, :].astype(jnp.float32) + relay[kind, step, half, rows, :].astype(jnp.float32)
                part[kind, step, piece, where, :] = value.astype(jnp.bfloat16)
                return carry

            lax.fori_loop(0, 4, add, 0)
            hop(kind, step, 4 + half).start()

    def middle(kind, step):
        f = first_axis(kind, step)
        wait_for(part_in.at[kind, step], one_sem.at[kind, step, 1])
        mine = one_pos(kind, f)

        def add(tile, carry):
            rows = pl.ds(pl.multiple_of(tile * 16, 16), 16)
            value = part[kind, step, mine, rows, :].astype(jnp.float32)
            for side in range(2):
                value = value + part_in[kind, step, side, rows, :].astype(jnp.float32)
            sums[kind, step, rows, :] = value.astype(jnp.bfloat16)
            return carry

        lax.fori_loop(0, 8, add, 0)
        for d in (2, 1, 3):
            two_copy(kind, step, d).start()

    def last(kind, step):
        f = first_axis(kind, step)
        mine = two_pos(kind, f)
        wait_for(sums_in.at[kind, step, pl.ds(0, 96), :], two_sem.at[kind, step])
        if kind == 0:
            value = sums[kind, step, quarter(mine), :].astype(jnp.float32)
            for d in range(1, 4):
                value = value + sums_in[kind, step, quarter(mine + d), :].astype(jnp.float32)
            out[0, pl.ds(pl.multiple_of(step * WA, WA), WA), :] = value
        else:
            for e in range(2):
                zl = lax.rem(low + e, 2)

                def rows(pos):
                    return pl.ds(pl.multiple_of(lax.rem(pos, 4) * 32 + zl * WB, WB), WB)

                value = sums[kind, step, rows(mine), :].astype(jnp.float32)
                for d in range(1, 4):
                    value = value + sums_in[kind, step, rows(mine + d), :].astype(jnp.float32)
                if e == 0:
                    out[0, row_b(low, step), :] = value
                else:
                    swap[step] = value
            swap_copy(step, low).start()

    def body(step, carry):
        @pl.when(step + AHEAD < STEPS)
        def _():
            for kind in range(2):
                send_slab(kind, step + AHEAD)

        for kind in range(2):
            produce(kind, step)

            @pl.when(step >= LAG0)
            def _():
                forward(kind, step - LAG0)

            @pl.when(step >= LAG1)
            def _():
                middle(kind, step - LAG1)

        @pl.when(step >= LAG2)
        def _():
            for kind in range(2):
                last(kind, step - LAG2)

        return carry

    lax.fori_loop(0, STEPS, body, 0)
    def finish(step, carry):
        @pl.when(step < STEPS + LAG0)
        def _():
            for kind in range(2):
                forward(kind, step - LAG0)

        @pl.when(step < STEPS + LAG1)
        def _():
            for kind in range(2):
                middle(kind, step - LAG1)

        for kind in range(2):
            last(kind, step - LAG2)
        return carry

    lax.fori_loop(STEPS, STEPS + LAG2, finish, 0)

    for kind in range(2):
        slab = slab_a if kind == 0 else slab_b
        wait_for(feats.at[kind, :, pl.ds(0, 896), :], feat_out.at[kind])
        wait_for(slab.at[:, :, :, :, pl.ds(0, 896)], slab_out.at[kind])
    wait_for(relay, one_out.at[0])
    wait_for(part_in, one_out.at[1])
    wait_for(sums_in.at[:, :, pl.ds(0, 96), :], two_out.at[0])
    wait_for(swap, swap_out.at[0])
    wait_for(swap, swap_sem.at[0])


def per_device(weight, activation, points):
    hbm = pl.BlockSpec(memory_space=pltpu.HBM)
    dma = pltpu.SemaphoreType.DMA
    return pl.pallas_call(
        kernel,
        out_shape=jax.ShapeDtypeStruct((1, 512, 512), jnp.float32),
        in_specs=[hbm, hbm, hbm],
        out_specs=pl.BlockSpec(memory_space=pltpu.VMEM),
        scratch_shapes=[
            pltpu.VMEM((STEPS, 4, 2, WA, 1024), jnp.bfloat16),
            pltpu.VMEM((STEPS, 4, 4, WB, 1024), jnp.bfloat16),
            pltpu.VMEM((2, 2, 1024, 512), jnp.bfloat16),
            pltpu.VMEM((2, 4, 64, 512), jnp.float32),
            pltpu.VMEM((2, STEPS, 4, 128, 512), jnp.bfloat16),
            pltpu.VMEM((2, STEPS, 2, 64, 512), jnp.bfloat16),
            pltpu.VMEM((2, STEPS, 2, 128, 512), jnp.bfloat16),
            pltpu.VMEM((2, STEPS, 128, 512), jnp.bfloat16),
            pltpu.VMEM((2, STEPS, 128, 512), jnp.bfloat16),
            pltpu.VMEM((STEPS, WB, 512), jnp.float32),
            pltpu.SMEM((8,), jnp.int32),
            dma((2, STEPS)), dma((2,)), dma((2, 3)), dma((2,)), dma((2,)),
            dma((2, STEPS, 2)), dma((2,)), dma((2, STEPS)), dma((1,)), dma((1,)), dma((1,)), dma((3,)),
        ],
        compiler_params=pltpu.CompilerParams(
            collective_id=0, has_side_effects=True, vmem_limit_bytes=52 * 2**20),
        name="coded_share",
    )(weight.reshape(4, 2, 4, 2, 512, 128), activation, points)


def solution(mesh):
    placed = (P(None, None, ("grp", "mem")), P(None, ("grp", "mem"), None), P())
    return jax.shard_map(
        per_device, mesh=mesh, in_specs=placed, out_specs=P("grp", "mem", None), check_vma=False
    )
```

```python
import jax
import jax.numpy as jnp
from jax import lax
from jax.experimental import pallas as pl
from jax.experimental.pallas import tpu as pltpu
from jax.sharding import PartitionSpec as P

MESH = pl.DeviceIdType.MESH
STEPS = 8
WA = 32
WB = 16
BASE_B = STEPS * WA
AHEAD = 8
OTHER_A = (5, 6)
OTHER_B = (5, 7)
LAG0 = 2
LAG1 = 5
LAG2 = 8


def place():
    grp, mem = lax.axis_index("grp"), lax.axis_index("mem")
    return grp // 2, (mem // 2) % 4, (mem // 8) * 2 + grp % 2, mem % 2


def device(x, y, z, core):
    return (x * 2 + z % 2, (z // 2) * 8 + y * 2 + core)


def kernel(weight, act, points, out, slab_a, slab_b, feats, prods, part, relay, part_in, sums, sums_in, swap, anchor_mem,
           slab_sem, slab_out, feat_sem, pair_sem, feat_out, one_sem, one_out, two_sem, two_out, swap_sem, swap_out,
           misc_sem):
    x, y, z, core = place()
    low = z % 2
    gather_order = [(d, e) for d in (2, 1, 3, 0) for e in (0, 1) if d or e]

    def at(xx, yy, zz, cc):
        return device(lax.rem(xx, 4), lax.rem(yy, 4), lax.rem(zz, 4), lax.rem(cc, 2))

    peers = [at(x, y + d, z, core + e) for d in range(4) for e in range(2) if d or e]
    peers += [at(x, y, z + d, core + e) for d in range(1, 4) for e in range(2)]
    peers += [at(x + d, y, z, core) for d in range(1, 4)]
    barrier = pltpu.get_barrier_semaphore()
    for peer in peers:
        pl.semaphore_signal(barrier, inc=1, device_id=peer, device_id_type=MESH)
    pl.semaphore_wait(barrier, len(peers))

    def wait_for(ref, sem):
        pltpu.make_async_copy(ref, ref, sem).wait()

    def lanes(index):
        return pl.ds(pl.multiple_of(index * 128, 128), 128)

    def line_at(kind, d, e):
        return at(x, y + d, z, core + e) if kind == 0 else at(x, y, z + d, core + e)

    def line_pos(kind):
        return y if kind == 0 else z

    def line_index(kind, d, e):
        return lax.rem(line_pos(kind) + d, 4) * 2 + lax.rem(core + e, 2)

    def feat_slot(kind, index):
        return feats.at[kind, :, lanes(index), :]

    def feat_send(kind, d):
        return pltpu.make_async_remote_copy(
            src_ref=act, dst_ref=feat_slot(kind, line_index(kind, 0, 0)), send_sem=feat_out.at[kind],
            recv_sem=feat_sem.at[kind, d - 1], device_id=line_at(kind, d, 0), device_id_type=MESH)

    def feat_pass(kind, d):
        index, half = line_index(kind, 4 - d, 0), d // 2
        piece = feats.at[kind, half, lanes(index), :]
        return pltpu.make_async_remote_copy(
            src_ref=piece, dst_ref=piece, send_sem=feat_out.at[kind],
            recv_sem=feat_sem.at[kind, 1], device_id=line_at(kind, d, 0), device_id_type=MESH)

    def feat_pair(kind, d):
        index = line_index(kind, d, 0)
        return pltpu.make_async_remote_copy(
            src_ref=act if d == 0 else feat_slot(kind, index), dst_ref=feat_slot(kind, index),
            send_sem=feat_out.at[kind], recv_sem=pair_sem.at[kind], device_id=line_at(kind, 0, 1), device_id_type=MESH)

    def rows_for(kind, step, d, e):
        pos, cc = lax.rem(line_pos(kind) + d, 4), lax.rem(core + e, 2)
        if kind == 0:
            start = pl.multiple_of(step * WA, WA)
            return weight.at[:, :, pos, cc, pl.ds(start, WA), :]
        start = pl.multiple_of(BASE_B + (pos % 2) * (STEPS * WB) + step * WB, WB)
        return weight.at[:, pos // 2, :, cc, pl.ds(start, WB), :]

    def slab_slot(kind, step, index):
        slab = slab_a if kind == 0 else slab_b
        return slab.at[step, :, :, :, lanes(index)]

    def slab_copy(kind, step, d, e):
        mine = line_index(kind, 0, 0)
        return pltpu.make_async_remote_copy(
            src_ref=rows_for(kind, step, d, e), dst_ref=slab_slot(kind, step, mine),
            send_sem=slab_out.at[kind], recv_sem=slab_sem.at[kind, step],
            device_id=line_at(kind, d, e), device_id_type=MESH)

    def slab_own(kind, step):
        return pltpu.make_async_copy(
            rows_for(kind, step, 0, 0), slab_slot(kind, step, line_index(kind, 0, 0)), slab_sem.at[kind, step])

    def send_slab(kind, step):
        slab_own(kind, step).start()
        for d, e in gather_order:
            slab_copy(kind, step, d, e).start()

    def first_axis(kind, step):
        other = OTHER_A if kind == 0 else OTHER_B
        flag = jnp.int32(1)
        for k in other:
            flag = flag - (step == k).astype(jnp.int32)
        return flag

    def one_pos(kind, f):
        return f * x + (1 - f) * (z if kind == 0 else y)

    def one_at(kind, f, d):
        if kind == 0:
            return at(x + f * d, y, z + (1 - f) * d, core)
        return at(x + f * d, y + (1 - f) * d, z, core)

    def hop(kind, step, order):
        f = first_axis(kind, step)
        mine = one_pos(kind, f)
        piece, half, way = ((2, 0, 1), (2, 1, 3), (1, 1, 1), (3, 0, 3), (1, 0, 1), (3, 1, 3))[order]
        rows = pl.ds(half * 64, 64)
        side = 0 if way == 1 else 1
        group = 0 if order < 2 else 1
        target = relay.at[kind, step, half] if order < 2 else part_in.at[kind, step, side, rows, :]
        return pltpu.make_async_remote_copy(
            src_ref=part.at[kind, step, lax.rem(mine + piece, 4), rows, :], dst_ref=target,
            send_sem=one_out.at[group], recv_sem=one_sem.at[kind, step, group],
            device_id=one_at(kind, f, way), device_id_type=MESH)

    def two_pos(kind, f):
        return f * (z if kind == 0 else y) + (1 - f) * x

    def two_at(kind, f, d):
        if kind == 0:
            return at(x + (1 - f) * d, y, z + f * d, core)
        return at(x + (1 - f) * d, y + f * d, z, core)

    def quarter(pos):
        return pl.ds(pl.multiple_of(lax.rem(pos, 4) * 32, 32), 32)

    def two_copy(kind, step, d):
        f = first_axis(kind, step)
        mine = two_pos(kind, f)
        return pltpu.make_async_remote_copy(
            src_ref=sums.at[kind, step, quarter(mine + d), :], dst_ref=sums_in.at[kind, step, quarter(mine), :],
            send_sem=two_out.at[0], recv_sem=two_sem.at[kind, step],
            device_id=two_at(kind, f, d), device_id_type=MESH)

    def row_b(which, step):
        return pl.ds(pl.multiple_of(BASE_B + which * (STEPS * WB) + step * WB, WB), WB)

    def swap_copy(step, which):
        rows = row_b(which, step)
        return pltpu.make_async_remote_copy(
            src_ref=swap.at[step], dst_ref=out.at[0, rows, :], send_sem=swap_out.at[0], recv_sem=swap_sem.at[0],
            device_id=at(x, y, (z // 2) * 2 + 1 - low, core), device_id_type=MESH)

    points_copy = pltpu.make_async_copy(points, anchor_mem, misc_sem.at[0])
    points_copy.start()
    own_feats = [pltpu.make_async_copy(act, feat_slot(kind, line_index(kind, 0, 0)), misc_sem.at[1 + kind]) for kind in range(2)]
    for d in (1, 3):
        for kind in range(2):
            feat_send(kind, d).start()
    for kind in range(2):
        own_feats[kind].start()
        feat_pair(kind, 0).start()
    for d in (1, 3):
        for kind in range(2):
            wait_for(feat_slot(kind, line_index(kind, 4 - d, 0)), feat_sem.at[kind, d - 1])
            feat_pass(kind, d).start()
    for d in (1, 3):
        for kind in range(2):
            feat_pair(kind, d).start()
    for step in range(AHEAD):
        for kind in range(2):
            send_slab(kind, step)
    for kind in range(2):
        wait_for(feat_slot(kind, line_index(kind, 2, 0)), feat_sem.at[kind, 1])
        feat_pair(kind, 2).start()
    points_copy.wait()
    for kind in range(2):
        own_feats[kind].wait()
        wait_for(feats.at[kind, :, pl.ds(0, 512), :], pair_sem.at[kind])

    anchors = [(anchor_mem[g] + 1).astype(jnp.float32) * 0.125 for g in range(8)]

    def produce(kind, step):
        f = first_axis(kind, step)
        slab = slab_a if kind == 0 else slab_b
        wait_for(slab.at[step], slab_sem.at[kind, step])
        left = slab[step].reshape(256, 1024)
        for k in range(2):
            prods[k] = jnp.dot(left, feats[kind, k], preferred_element_type=jnp.float32).reshape(4, 64, 512)

        def combine(tile, carry):
            rows = pl.ds(pl.multiple_of(tile * 16, 16), 16)
            for half in range(2):
                cols = pl.ds(half * 256, 256)
                terms = [prods[p // 4, p % 4, rows, cols] for p in range(8)]
                for g in range(8):
                    value = terms[7]
                    for p in range(6, -1, -1):
                        value = value * anchors[g] + terms[p]
                    gx, zl = g // 2, g % 2
                    if kind == 0:
                        zz, inner = (tile // 2) * 2 + zl, (tile % 2) * 16
                        owner = f * gx + (1 - f) * zz
                        row = (f * zz + (1 - f) * gx) * WA + inner
                    else:
                        owner = f * gx + (1 - f) * tile
                        row = (f * tile + (1 - f) * gx) * 32 + zl * WB
                    part[kind, step, owner, pl.ds(pl.multiple_of(row, 16), 16), cols] = value.astype(jnp.bfloat16)
            return carry

        lax.fori_loop(0, 4, combine, 0)
        for order in range(4):
            hop(kind, step, order).start()

    def forward(kind, step):
        f = first_axis(kind, step)
        mine = one_pos(kind, f)
        wait_for(relay.at[kind, step], one_sem.at[kind, step, 0])
        for half in range(2):
            piece = lax.rem(mine + (1 if half == 0 else 3), 4)

            def add(tile, carry):
                rows = pl.ds(pl.multiple_of(tile * 16, 16), 16)
                where = pl.ds(pl.multiple_of(half * 64 + tile * 16, 16), 16)
                value = part[kind, step, piece, where, :].astype(jnp.float32) + relay[kind, step, half, rows, :].astype(jnp.float32)
                part[kind, step, piece, where, :] = value.astype(jnp.bfloat16)
                return carry

            lax.fori_loop(0, 4, add, 0)
            hop(kind, step, 4 + half).start()

    def middle(kind, step):
        f = first_axis(kind, step)
        wait_for(part_in.at[kind, step], one_sem.at[kind, step, 1])
        mine = one_pos(kind, f)

        def add(tile, carry):
            rows = pl.ds(pl.multiple_of(tile * 16, 16), 16)
            value = part[kind, step, mine, rows, :].astype(jnp.float32)
            for side in range(2):
                value = value + part_in[kind, step, side, rows, :].astype(jnp.float32)
            sums[kind, step, rows, :] = value.astype(jnp.bfloat16)
            return carry

        lax.fori_loop(0, 8, add, 0)
        for d in (2, 1, 3):
            two_copy(kind, step, d).start()

    def last(kind, step):
        f = first_axis(kind, step)
        mine = two_pos(kind, f)
        wait_for(sums_in.at[kind, step, pl.ds(0, 96), :], two_sem.at[kind, step])
        if kind == 0:
            value = sums[kind, step, quarter(mine), :].astype(jnp.float32)
            for d in range(1, 4):
                value = value + sums_in[kind, step, quarter(mine + d), :].astype(jnp.float32)
            out[0, pl.ds(pl.multiple_of(step * WA, WA), WA), :] = value
        else:
            for e in range(2):
                zl = lax.rem(low + e, 2)

                def rows(pos):
                    return pl.ds(pl.multiple_of(lax.rem(pos, 4) * 32 + zl * WB, WB), WB)

                value = sums[kind, step, rows(mine), :].astype(jnp.float32)
                for d in range(1, 4):
                    value = value + sums_in[kind, step, rows(mine + d), :].astype(jnp.float32)
                if e == 0:
                    out[0, row_b(low, step), :] = value
                else:
                    swap[step] = value
            swap_copy(step, low).start()

    def body(step, carry):
        @pl.when(step + AHEAD < STEPS)
        def _():
            for kind in range(2):
                send_slab(kind, step + AHEAD)

        for kind in (1, 0):
            produce(kind, step)

            @pl.when(step >= LAG0)
            def _():
                forward(kind, step - LAG0)

            @pl.when(step >= LAG1)
            def _():
                middle(kind, step - LAG1)

        @pl.when(step >= LAG2)
        def _():
            for kind in range(2):
                last(kind, step - LAG2)

        return carry

    lax.fori_loop(0, STEPS, body, 0)
    def finish(step, carry):
        @pl.when(step < STEPS + LAG0)
        def _():
            for kind in (1, 0):
                forward(kind, step - LAG0)

        @pl.when(step < STEPS + LAG1)
        def _():
            for kind in (1, 0):
                middle(kind, step - LAG1)

        for kind in (1, 0):
            last(kind, step - LAG2)
        return carry

    lax.fori_loop(STEPS, STEPS + LAG2, finish, 0)

    for kind in range(2):
        slab = slab_a if kind == 0 else slab_b
        wait_for(feats.at[kind, :, pl.ds(0, 896), :], feat_out.at[kind])
        wait_for(slab.at[:, :, :, :, pl.ds(0, 896)], slab_out.at[kind])
    wait_for(relay, one_out.at[0])
    wait_for(part_in, one_out.at[1])
    wait_for(sums_in.at[:, :, pl.ds(0, 96), :], two_out.at[0])
    wait_for(swap, swap_out.at[0])
    wait_for(swap, swap_sem.at[0])


def per_device(weight, activation, points):
    hbm = pl.BlockSpec(memory_space=pltpu.HBM)
    dma = pltpu.SemaphoreType.DMA
    return pl.pallas_call(
        kernel,
        out_shape=jax.ShapeDtypeStruct((1, 512, 512), jnp.float32),
        in_specs=[hbm, hbm, hbm],
        out_specs=pl.BlockSpec(memory_space=pltpu.VMEM),
        scratch_shapes=[
            pltpu.VMEM((STEPS, 4, 2, WA, 1024), jnp.bfloat16),
            pltpu.VMEM((STEPS, 4, 4, WB, 1024), jnp.bfloat16),
            pltpu.VMEM((2, 2, 1024, 512), jnp.bfloat16),
            pltpu.VMEM((2, 4, 64, 512), jnp.float32),
            pltpu.VMEM((2, STEPS, 4, 128, 512), jnp.bfloat16),
            pltpu.VMEM((2, STEPS, 2, 64, 512), jnp.bfloat16),
            pltpu.VMEM((2, STEPS, 2, 128, 512), jnp.bfloat16),
            pltpu.VMEM((2, STEPS, 128, 512), jnp.bfloat16),
            pltpu.VMEM((2, STEPS, 128, 512), jnp.bfloat16),
            pltpu.VMEM((STEPS, WB, 512), jnp.float32),
            pltpu.SMEM((8,), jnp.int32),
            dma((2, STEPS)), dma((2,)), dma((2, 3)), dma((2,)), dma((2,)),
            dma((2, STEPS, 2)), dma((2,)), dma((2, STEPS)), dma((1,)), dma((1,)), dma((1,)), dma((3,)),
        ],
        compiler_params=pltpu.CompilerParams(
            collective_id=0, has_side_effects=True, vmem_limit_bytes=52 * 2**20),
        name="coded_share",
    )(weight.reshape(4, 2, 4, 2, 512, 128), activation, points)


def solution(mesh):
    placed = (P(None, None, ("grp", "mem")), P(None, ("grp", "mem"), None), P())
    return jax.shard_map(
        per_device, mesh=mesh, in_specs=placed, out_specs=P("grp", "mem", None), check_vma=False
    )
```

```python
import jax
import jax.numpy as jnp
from jax import lax
from jax.experimental import pallas as pl
from jax.experimental.pallas import tpu as pltpu
from jax.sharding import PartitionSpec as P

MESH = pl.DeviceIdType.MESH
STEPS = 8
WA = 32
WB = 16
BASE_B = STEPS * WA
AHEAD = 8
OTHER_A = (5, 6, 7)
OTHER_B = (5, 7)
LAG0 = 2
LAG1 = 5
LAG2 = 8


def place():
    grp, mem = lax.axis_index("grp"), lax.axis_index("mem")
    return grp // 2, (mem // 2) % 4, (mem // 8) * 2 + grp % 2, mem % 2


def device(x, y, z, core):
    return (x * 2 + z % 2, (z // 2) * 8 + y * 2 + core)


def kernel(weight, act, points, out, slab_a, slab_b, feats, prods, part, relay, part_in, sums, sums_in, swap, swap_in, anchor_mem,
           slab_sem, slab_out, feat_sem, pair_sem, feat_out, one_sem, one_out, two_sem, two_out, swap_sem, swap_out,
           misc_sem):
    x, y, z, core = place()
    low = z % 2
    early = ((1, 0), (3, 0))
    gather_order = [(d, e) for d in (2, 1, 3, 0) for e in (0, 1) if d or e]

    def at(xx, yy, zz, cc):
        return device(lax.rem(xx, 4), lax.rem(yy, 4), lax.rem(zz, 4), lax.rem(cc, 2))

    peers = [at(x, y + d, z, core + e) for d in range(4) for e in range(2) if d or e]
    peers += [at(x, y, z + d, core + e) for d in range(1, 4) for e in range(2)]
    peers += [at(x + d, y, z, core) for d in range(1, 4)]
    barrier = pltpu.get_barrier_semaphore()
    for peer in peers:
        pl.semaphore_signal(barrier, inc=1, device_id=peer, device_id_type=MESH)
    pl.semaphore_wait(barrier, len(peers))

    def wait_for(ref, sem):
        pltpu.make_async_copy(ref, ref, sem).wait()

    def lanes(index):
        return pl.ds(pl.multiple_of(index * 128, 128), 128)

    def line_at(kind, d, e):
        return at(x, y + d, z, core + e) if kind == 0 else at(x, y, z + d, core + e)

    def line_pos(kind):
        return y if kind == 0 else z

    def line_index(kind, d, e):
        return lax.rem(line_pos(kind) + d, 4) * 2 + lax.rem(core + e, 2)

    def feat_slot(kind, index):
        return feats.at[kind, :, lanes(index), :]

    def feat_send(kind, d):
        return pltpu.make_async_remote_copy(
            src_ref=act, dst_ref=feat_slot(kind, line_index(kind, 0, 0)), send_sem=feat_out.at[kind],
            recv_sem=feat_sem.at[kind, d - 1], device_id=line_at(kind, d, 0), device_id_type=MESH)

    def feat_pass(kind, d):
        index, half = line_index(kind, 4 - d, 0), d // 2
        piece = feats.at[kind, half, lanes(index), :]
        return pltpu.make_async_remote_copy(
            src_ref=piece, dst_ref=piece, send_sem=feat_out.at[kind],
            recv_sem=feat_sem.at[kind, 1], device_id=line_at(kind, d, 0), device_id_type=MESH)

    def feat_pair(kind, d):
        index = line_index(kind, d, 0)
        return pltpu.make_async_remote_copy(
            src_ref=act if d == 0 else feat_slot(kind, index), dst_ref=feat_slot(kind, index),
            send_sem=feat_out.at[kind], recv_sem=pair_sem.at[kind], device_id=line_at(kind, 0, 1), device_id_type=MESH)

    def rows_for(kind, step, d, e):
        pos, cc = lax.rem(line_pos(kind) + d, 4), lax.rem(core + e, 2)
        if kind == 0:
            start = pl.multiple_of(step * WA, WA)
            return weight.at[:, :, pos, cc, pl.ds(start, WA), :]
        start = pl.multiple_of(BASE_B + (pos % 2) * (STEPS * WB) + step * WB, WB)
        return weight.at[:, pos // 2, :, cc, pl.ds(start, WB), :]

    def slab_slot(kind, step, index):
        slab = slab_a if kind == 0 else slab_b
        return slab.at[step, :, :, :, lanes(index)]

    def slab_copy(kind, step, d, e):
        mine = line_index(kind, 0, 0)
        return pltpu.make_async_remote_copy(
            src_ref=rows_for(kind, step, d, e), dst_ref=slab_slot(kind, step, mine),
            send_sem=slab_out.at[kind], recv_sem=slab_sem.at[kind, step],
            device_id=line_at(kind, d, e), device_id_type=MESH)

    def slab_own(kind, step):
        return pltpu.make_async_copy(
            rows_for(kind, step, 0, 0), slab_slot(kind, step, line_index(kind, 0, 0)), slab_sem.at[kind, step])

    def send_slab(kind, step):
        slab_own(kind, step).start()
        for d, e in gather_order:
            slab_copy(kind, step, d, e).start()

    def first_axis(kind, step):
        other = OTHER_A if kind == 0 else OTHER_B
        flag = jnp.int32(1)
        for k in other:
            flag = flag - (step == k).astype(jnp.int32)
        return flag

    def one_pos(kind, f):
        return f * x + (1 - f) * (z if kind == 0 else y)

    def one_at(kind, f, d):
        if kind == 0:
            return at(x + f * d, y, z + (1 - f) * d, core)
        return at(x + f * d, y + (1 - f) * d, z, core)

    def hop(kind, step, order):
        f = first_axis(kind, step)
        mine = one_pos(kind, f)
        piece, half, way = ((2, 0, 1), (2, 1, 3), (1, 1, 1), (3, 0, 3), (1, 0, 1), (3, 1, 3))[order]
        rows = pl.ds(half * 64, 64)
        side = 0 if way == 1 else 1
        group = 0 if order < 2 else 1
        target = relay.at[kind, step, half] if order < 2 else part_in.at[kind, step, side, rows, :]
        return pltpu.make_async_remote_copy(
            src_ref=part.at[kind, step, lax.rem(mine + piece, 4), rows, :], dst_ref=target,
            send_sem=one_out.at[group], recv_sem=one_sem.at[kind, step, group],
            device_id=one_at(kind, f, way), device_id_type=MESH)

    def two_pos(kind, f):
        return f * (z if kind == 0 else y) + (1 - f) * x

    def two_at(kind, f, d):
        if kind == 0:
            return at(x + (1 - f) * d, y, z + f * d, core)
        return at(x + (1 - f) * d, y + f * d, z, core)

    def quarter(pos):
        return pl.ds(pl.multiple_of(lax.rem(pos, 4) * 32, 32), 32)

    def two_copy(kind, step, d):
        f = first_axis(kind, step)
        mine = two_pos(kind, f)
        return pltpu.make_async_remote_copy(
            src_ref=sums.at[kind, step, quarter(mine + d), :], dst_ref=sums_in.at[kind, step, quarter(mine), :],
            send_sem=two_out.at[0], recv_sem=two_sem.at[kind, step],
            device_id=two_at(kind, f, d), device_id_type=MESH)

    def row_b(which, step):
        return pl.ds(pl.multiple_of(BASE_B + which * (STEPS * WB) + step * WB, WB), WB)

    def swap_copy(step):
        return pltpu.make_async_remote_copy(
            src_ref=swap.at[step], dst_ref=swap_in.at[step], send_sem=swap_out.at[0], recv_sem=swap_sem.at[0],
            device_id=at(x, y, (z // 2) * 2 + 1 - low, core), device_id_type=MESH)

    points_copy = pltpu.make_async_copy(points, anchor_mem, misc_sem.at[0])
    points_copy.start()
    own_feats = [pltpu.make_async_copy(act, feat_slot(kind, line_index(kind, 0, 0)), misc_sem.at[1 + kind]) for kind in range(2)]
    for d in (1, 3):
        for kind in range(2):
            feat_send(kind, d).start()
    for kind in range(2):
        own_feats[kind].start()
        feat_pair(kind, 0).start()
    for d, e in early:
        for kind in range(2):
            slab_copy(kind, 0, d, e).start()
    for d in (1, 3):
        for kind in range(2):
            wait_for(feat_slot(kind, line_index(kind, 4 - d, 0)), feat_sem.at[kind, d - 1])
            feat_pass(kind, d).start()
    for d in (1, 3):
        for kind in range(2):
            feat_pair(kind, d).start()
    for kind in range(2):
        slab_own(kind, 0).start()
        for d, e in gather_order:
            if (d, e) not in early:
                slab_copy(kind, 0, d, e).start()
    for step in range(1, AHEAD):
        for kind in range(2):
            send_slab(kind, step)
    for kind in range(2):
        wait_for(feat_slot(kind, line_index(kind, 2, 0)), feat_sem.at[kind, 1])
        feat_pair(kind, 2).start()
    points_copy.wait()
    for kind in range(2):
        own_feats[kind].wait()
        wait_for(feats.at[kind, :, pl.ds(0, 512), :], pair_sem.at[kind])

    anchors = [(anchor_mem[g] + 1).astype(jnp.float32) * 0.125 for g in range(8)]

    def produce(kind, step):
        f = first_axis(kind, step)
        slab = slab_a if kind == 0 else slab_b
        wait_for(slab.at[step], slab_sem.at[kind, step])
        left = slab[step].reshape(256, 1024)
        for k in range(2):
            prods[k] = jnp.dot(left, feats[kind, k], preferred_element_type=jnp.float32).reshape(4, 64, 512)

        def combine(tile, carry):
            rows = pl.ds(pl.multiple_of(tile * 16, 16), 16)
            for half in range(2):
                cols = pl.ds(half * 256, 256)
                terms = [prods[p // 4, p % 4, rows, cols] for p in range(8)]
                for g in range(8):
                    value = terms[7]
                    for p in range(6, -1, -1):
                        value = value * anchors[g] + terms[p]
                    gx, zl = g // 2, g % 2
                    if kind == 0:
                        zz, inner = (tile // 2) * 2 + zl, (tile % 2) * 16
                        owner = f * gx + (1 - f) * zz
                        row = (f * zz + (1 - f) * gx) * WA + inner
                    else:
                        owner = f * gx + (1 - f) * tile
                        row = (f * tile + (1 - f) * gx) * 32 + zl * WB
                    part[kind, step, owner, pl.ds(pl.multiple_of(row, 16), 16), cols] = value.astype(jnp.bfloat16)
            return carry

        lax.fori_loop(0, 4, combine, 0)
        for order in range(4):
            hop(kind, step, order).start()

    def forward(kind, step):
        f = first_axis(kind, step)
        mine = one_pos(kind, f)
        wait_for(relay.at[kind, step], one_sem.at[kind, step, 0])
        for half in range(2):
            piece = lax.rem(mine + (1 if half == 0 else 3), 4)

            def add(tile, carry):
                rows = pl.ds(pl.multiple_of(tile * 16, 16), 16)
                where = pl.ds(pl.multiple_of(half * 64 + tile * 16, 16), 16)
                value = part[kind, step, piece, where, :].astype(jnp.float32) + relay[kind, step, half, rows, :].astype(jnp.float32)
                part[kind, step, piece, where, :] = value.astype(jnp.bfloat16)
                return carry

            lax.fori_loop(0, 4, add, 0)
            hop(kind, step, 4 + half).start()

    def middle(kind, step):
        f = first_axis(kind, step)
        wait_for(part_in.at[kind, step], one_sem.at[kind, step, 1])
        mine = one_pos(kind, f)

        def add(tile, carry):
            rows = pl.ds(pl.multiple_of(tile * 16, 16), 16)
            value = part[kind, step, mine, rows, :].astype(jnp.float32)
            for side in range(2):
                value = value + part_in[kind, step, side, rows, :].astype(jnp.float32)
            sums[kind, step, rows, :] = value.astype(jnp.bfloat16)
            return carry

        lax.fori_loop(0, 8, add, 0)
        for d in (2, 1, 3):
            two_copy(kind, step, d).start()

    def last(kind, step):
        f = first_axis(kind, step)
        mine = two_pos(kind, f)
        wait_for(sums_in.at[kind, step, pl.ds(0, 96), :], two_sem.at[kind, step])
        if kind == 0:
            value = sums[kind, step, quarter(mine), :].astype(jnp.float32)
            for d in range(1, 4):
                value = value + sums_in[kind, step, quarter(mine + d), :].astype(jnp.float32)
            out[0, pl.ds(pl.multiple_of(step * WA, WA), WA), :] = value
        else:
            for e in range(2):
                zl = lax.rem(low + e, 2)

                def rows(pos):
                    return pl.ds(pl.multiple_of(lax.rem(pos, 4) * 32 + zl * WB, WB), WB)

                value = sums[kind, step, rows(mine), :].astype(jnp.float32)
                for d in range(1, 4):
                    value = value + sums_in[kind, step, rows(mine + d), :].astype(jnp.float32)
                if e == 0:
                    out[0, row_b(low, step), :] = value
                else:
                    swap[step] = value.astype(jnp.bfloat16)
            swap_copy(step).start()

    def body(step, carry):
        @pl.when(step + AHEAD < STEPS)
        def _():
            for kind in range(2):
                send_slab(kind, step + AHEAD)

        for kind in (1, 0):
            produce(kind, step)

            @pl.when(step >= LAG0)
            def _():
                forward(kind, step - LAG0)

            @pl.when(step >= LAG1)
            def _():
                middle(kind, step - LAG1)

        @pl.when(step >= LAG2)
        def _():
            for kind in range(2):
                last(kind, step - LAG2)

        return carry

    lax.fori_loop(0, STEPS, body, 0)
    def finish(step, carry):
        @pl.when(step < STEPS + LAG0)
        def _():
            for kind in (1, 0):
                forward(kind, step - LAG0)

        @pl.when(step < STEPS + LAG1)
        def _():
            for kind in (1, 0):
                middle(kind, step - LAG1)

        for kind in (1, 0):
            last(kind, step - LAG2)
        return carry

    lax.fori_loop(STEPS, STEPS + LAG2, finish, 0)

    for kind in range(2):
        slab = slab_a if kind == 0 else slab_b
        wait_for(feats.at[kind, :, pl.ds(0, 896), :], feat_out.at[kind])
        wait_for(slab.at[:, :, :, :, pl.ds(0, 896)], slab_out.at[kind])
    wait_for(relay, one_out.at[0])
    wait_for(part_in, one_out.at[1])
    wait_for(sums_in.at[:, :, pl.ds(0, 96), :], two_out.at[0])
    wait_for(swap, swap_out.at[0])
    wait_for(swap_in, swap_sem.at[0])
    half = pl.ds(pl.multiple_of(BASE_B + (1 - low) * (STEPS * WB), WB), STEPS * WB)
    out[0, half, :] = swap_in[...].reshape(STEPS * WB, 512).astype(jnp.float32)


def per_device(weight, activation, points):
    hbm = pl.BlockSpec(memory_space=pltpu.HBM)
    dma = pltpu.SemaphoreType.DMA
    return pl.pallas_call(
        kernel,
        out_shape=jax.ShapeDtypeStruct((1, 512, 512), jnp.float32),
        in_specs=[hbm, hbm, hbm],
        out_specs=pl.BlockSpec(memory_space=pltpu.VMEM),
        scratch_shapes=[
            pltpu.VMEM((STEPS, 4, 2, WA, 1024), jnp.bfloat16),
            pltpu.VMEM((STEPS, 4, 4, WB, 1024), jnp.bfloat16),
            pltpu.VMEM((2, 2, 1024, 512), jnp.bfloat16),
            pltpu.VMEM((2, 4, 64, 512), jnp.float32),
            pltpu.VMEM((2, STEPS, 4, 128, 512), jnp.bfloat16),
            pltpu.VMEM((2, STEPS, 2, 64, 512), jnp.bfloat16),
            pltpu.VMEM((2, STEPS, 2, 128, 512), jnp.bfloat16),
            pltpu.VMEM((2, STEPS, 128, 512), jnp.bfloat16),
            pltpu.VMEM((2, STEPS, 128, 512), jnp.bfloat16),
            pltpu.VMEM((STEPS, WB, 512), jnp.bfloat16),
            pltpu.VMEM((STEPS, WB, 512), jnp.bfloat16),
            pltpu.SMEM((8,), jnp.int32),
            dma((2, STEPS)), dma((2,)), dma((2, 3)), dma((2,)), dma((2,)),
            dma((2, STEPS, 2)), dma((2,)), dma((2, STEPS)), dma((1,)), dma((1,)), dma((1,)), dma((3,)),
        ],
        compiler_params=pltpu.CompilerParams(
            collective_id=0, has_side_effects=True, vmem_limit_bytes=52 * 2**20),
        name="coded_share",
    )(weight.reshape(4, 2, 4, 2, 512, 128), activation, points)


def solution(mesh):
    placed = (P(None, None, ("grp", "mem")), P(None, ("grp", "mem"), None), P())
    return jax.shard_map(
        per_device, mesh=mesh, in_specs=placed, out_specs=P("grp", "mem", None), check_vma=False
    )
```

```python
import jax
import jax.numpy as jnp
from jax import lax
from jax.experimental import pallas as pl
from jax.experimental.pallas import tpu as pltpu
from jax.sharding import PartitionSpec as P

MESH = pl.DeviceIdType.MESH
STEPS = 8
WA = 32
WB = 16
BASE_B = STEPS * WA
AHEAD = 8
OTHER_A = (5, 6, 7)
OTHER_B = (5, 7)
LAG0 = 2
LAG1 = 5
LAG2 = 8


def place():
    grp, mem = lax.axis_index("grp"), lax.axis_index("mem")
    return grp // 2, (mem // 2) % 4, (mem // 8) * 2 + grp % 2, mem % 2


def device(x, y, z, core):
    return (x * 2 + z % 2, (z // 2) * 8 + y * 2 + core)


def kernel(weight, act, points, out, slab_a, slab_b, feats, prods, part, relay, part_in, sums, sums_in, swap, swap_in, anchor_mem,
           slab_sem, slab_out, feat_sem, pair_sem, feat_out, one_sem, one_out, two_sem, two_out, swap_sem, swap_out,
           misc_sem):
    x, y, z, core = place()
    low = z % 2
    early = ((1, 0), (3, 0))
    gather_order = [(d, e) for d in (2, 1, 3, 0) for e in (0, 1) if d or e]

    def at(xx, yy, zz, cc):
        return device(lax.rem(xx, 4), lax.rem(yy, 4), lax.rem(zz, 4), lax.rem(cc, 2))

    peers = [at(x, y + d, z, core + e) for d in range(4) for e in range(2) if d or e]
    peers += [at(x, y, z + d, core + e) for d in range(1, 4) for e in range(2)]
    peers += [at(x + d, y, z, core) for d in range(1, 4)]
    barrier = pltpu.get_barrier_semaphore()
    for peer in peers:
        pl.semaphore_signal(barrier, inc=1, device_id=peer, device_id_type=MESH)

    def wait_for(ref, sem):
        pltpu.make_async_copy(ref, ref, sem).wait()

    def lanes(index):
        return pl.ds(pl.multiple_of(index * 128, 128), 128)

    def line_at(kind, d, e):
        return at(x, y + d, z, core + e) if kind == 0 else at(x, y, z + d, core + e)

    def line_pos(kind):
        return y if kind == 0 else z

    def line_index(kind, d, e):
        return lax.rem(line_pos(kind) + d, 4) * 2 + lax.rem(core + e, 2)

    def feat_slot(kind, index):
        return feats.at[kind, :, lanes(index), :]

    def feat_send(kind, d):
        return pltpu.make_async_remote_copy(
            src_ref=act, dst_ref=feat_slot(kind, line_index(kind, 0, 0)), send_sem=feat_out.at[kind],
            recv_sem=feat_sem.at[kind, d - 1], device_id=line_at(kind, d, 0), device_id_type=MESH)

    def feat_pass(kind, d):
        index, half = line_index(kind, 4 - d, 0), d // 2
        piece = feats.at[kind, half, lanes(index), :]
        return pltpu.make_async_remote_copy(
            src_ref=piece, dst_ref=piece, send_sem=feat_out.at[kind],
            recv_sem=feat_sem.at[kind, 1], device_id=line_at(kind, d, 0), device_id_type=MESH)

    def feat_pair(kind, d):
        index = line_index(kind, d, 0)
        return pltpu.make_async_remote_copy(
            src_ref=act if d == 0 else feat_slot(kind, index), dst_ref=feat_slot(kind, index),
            send_sem=feat_out.at[kind], recv_sem=pair_sem.at[kind], device_id=line_at(kind, 0, 1), device_id_type=MESH)

    def rows_for(kind, step, d, e):
        pos, cc = lax.rem(line_pos(kind) + d, 4), lax.rem(core + e, 2)
        if kind == 0:
            start = pl.multiple_of(step * WA, WA)
            return weight.at[:, :, pos, cc, pl.ds(start, WA), :]
        start = pl.multiple_of(BASE_B + (pos % 2) * (STEPS * WB) + step * WB, WB)
        return weight.at[:, pos // 2, :, cc, pl.ds(start, WB), :]

    def slab_slot(kind, step, index):
        slab = slab_a if kind == 0 else slab_b
        return slab.at[step, :, :, :, lanes(index)]

    def slab_copy(kind, step, d, e):
        mine = line_index(kind, 0, 0)
        return pltpu.make_async_remote_copy(
            src_ref=rows_for(kind, step, d, e), dst_ref=slab_slot(kind, step, mine),
            send_sem=slab_out.at[kind], recv_sem=slab_sem.at[kind, step],
            device_id=line_at(kind, d, e), device_id_type=MESH)

    def slab_own(kind, step):
        return pltpu.make_async_copy(
            rows_for(kind, step, 0, 0), slab_slot(kind, step, line_index(kind, 0, 0)), slab_sem.at[kind, step])

    def send_slab(kind, step):
        slab_own(kind, step).start()
        for d, e in gather_order:
            slab_copy(kind, step, d, e).start()

    def first_axis(kind, step):
        other = OTHER_A if kind == 0 else OTHER_B
        flag = jnp.int32(1)
        for k in other:
            flag = flag - (step == k).astype(jnp.int32)
        return flag

    def one_pos(kind, f):
        return f * x + (1 - f) * (z if kind == 0 else y)

    def one_at(kind, f, d):
        if kind == 0:
            return at(x + f * d, y, z + (1 - f) * d, core)
        return at(x + f * d, y + (1 - f) * d, z, core)

    def hop(kind, step, order):
        f = first_axis(kind, step)
        mine = one_pos(kind, f)
        piece, half, way = ((2, 0, 1), (2, 1, 3), (1, 1, 1), (3, 0, 3), (1, 0, 1), (3, 1, 3))[order]
        rows = pl.ds(half * 64, 64)
        side = 0 if way == 1 else 1
        group = 0 if order < 2 else 1
        target = relay.at[kind, step, half] if order < 2 else part_in.at[kind, step, side, rows, :]
        return pltpu.make_async_remote_copy(
            src_ref=part.at[kind, step, lax.rem(mine + piece, 4), rows, :], dst_ref=target,
            send_sem=one_out.at[group], recv_sem=one_sem.at[kind, step, group],
            device_id=one_at(kind, f, way), device_id_type=MESH)

    def two_pos(kind, f):
        return f * (z if kind == 0 else y) + (1 - f) * x

    def two_at(kind, f, d):
        if kind == 0:
            return at(x + (1 - f) * d, y, z + f * d, core)
        return at(x + (1 - f) * d, y + f * d, z, core)

    def quarter(pos):
        return pl.ds(pl.multiple_of(lax.rem(pos, 4) * 32, 32), 32)

    def two_copy(kind, step, d):
        f = first_axis(kind, step)
        mine = two_pos(kind, f)
        return pltpu.make_async_remote_copy(
            src_ref=sums.at[kind, step, quarter(mine + d), :], dst_ref=sums_in.at[kind, step, quarter(mine), :],
            send_sem=two_out.at[0], recv_sem=two_sem.at[kind, step],
            device_id=two_at(kind, f, d), device_id_type=MESH)

    def row_b(which, step):
        return pl.ds(pl.multiple_of(BASE_B + which * (STEPS * WB) + step * WB, WB), WB)

    def swap_copy(step):
        return pltpu.make_async_remote_copy(
            src_ref=swap.at[step], dst_ref=swap_in.at[step], send_sem=swap_out.at[0], recv_sem=swap_sem.at[0],
            device_id=at(x, y, (z // 2) * 2 + 1 - low, core), device_id_type=MESH)

    points_copy = pltpu.make_async_copy(points, anchor_mem, misc_sem.at[0])
    points_copy.start()
    own_feats = [pltpu.make_async_copy(act, feat_slot(kind, line_index(kind, 0, 0)), misc_sem.at[1 + kind]) for kind in range(2)]
    for kind in range(2):
        own_feats[kind].start()
        slab_own(kind, 0).start()
    pl.semaphore_wait(barrier, len(peers))
    for d in (1, 3):
        for kind in range(2):
            feat_send(kind, d).start()
    for kind in range(2):
        feat_pair(kind, 0).start()
    for d, e in early:
        for kind in range(2):
            slab_copy(kind, 0, d, e).start()
    for d in (1, 3):
        for kind in range(2):
            wait_for(feat_slot(kind, line_index(kind, 4 - d, 0)), feat_sem.at[kind, d - 1])
            feat_pass(kind, d).start()
    for d in (1, 3):
        for kind in range(2):
            feat_pair(kind, d).start()
    for kind in range(2):
        for d, e in gather_order:
            if (d, e) not in early:
                slab_copy(kind, 0, d, e).start()
    for step in range(1, AHEAD):
        for kind in range(2):
            send_slab(kind, step)
    for kind in range(2):
        wait_for(feat_slot(kind, line_index(kind, 2, 0)), feat_sem.at[kind, 1])
        feat_pair(kind, 2).start()
    points_copy.wait()
    for kind in range(2):
        own_feats[kind].wait()
        wait_for(feats.at[kind, :, pl.ds(0, 512), :], pair_sem.at[kind])

    anchors = [(anchor_mem[g] + 1).astype(jnp.float32) * 0.125 for g in range(8)]

    def produce(kind, step):
        f = first_axis(kind, step)
        slab = slab_a if kind == 0 else slab_b
        wait_for(slab.at[step], slab_sem.at[kind, step])
        left = slab[step].reshape(256, 1024)
        for k in range(2):
            prods[k] = jnp.dot(left, feats[kind, k], preferred_element_type=jnp.float32).reshape(4, 64, 512)

        def combine(tile, carry):
            rows = pl.ds(pl.multiple_of(tile * 16, 16), 16)
            for half in range(2):
                cols = pl.ds(half * 256, 256)
                terms = [prods[p // 4, p % 4, rows, cols] for p in range(8)]
                for g in range(8):
                    value = terms[7]
                    for p in range(6, -1, -1):
                        value = value * anchors[g] + terms[p]
                    gx, zl = g // 2, g % 2
                    if kind == 0:
                        zz, inner = (tile // 2) * 2 + zl, (tile % 2) * 16
                        owner = f * gx + (1 - f) * zz
                        row = (f * zz + (1 - f) * gx) * WA + inner
                    else:
                        owner = f * gx + (1 - f) * tile
                        row = (f * tile + (1 - f) * gx) * 32 + zl * WB
                    part[kind, step, owner, pl.ds(pl.multiple_of(row, 16), 16), cols] = value.astype(jnp.bfloat16)
            return carry

        lax.fori_loop(0, 4, combine, 0)
        for order in range(4):
            hop(kind, step, order).start()

    def forward(kind, step):
        f = first_axis(kind, step)
        mine = one_pos(kind, f)
        wait_for(relay.at[kind, step], one_sem.at[kind, step, 0])
        for half in range(2):
            piece = lax.rem(mine + (1 if half == 0 else 3), 4)

            def add(tile, carry):
                rows = pl.ds(pl.multiple_of(tile * 16, 16), 16)
                where = pl.ds(pl.multiple_of(half * 64 + tile * 16, 16), 16)
                value = part[kind, step, piece, where, :].astype(jnp.float32) + relay[kind, step, half, rows, :].astype(jnp.float32)
                part[kind, step, piece, where, :] = value.astype(jnp.bfloat16)
                return carry

            lax.fori_loop(0, 4, add, 0)
            hop(kind, step, 4 + half).start()

    def middle(kind, step):
        f = first_axis(kind, step)
        wait_for(part_in.at[kind, step], one_sem.at[kind, step, 1])
        mine = one_pos(kind, f)

        def add(tile, carry):
            rows = pl.ds(pl.multiple_of(tile * 16, 16), 16)
            value = part[kind, step, mine, rows, :].astype(jnp.float32)
            for side in range(2):
                value = value + part_in[kind, step, side, rows, :].astype(jnp.float32)
            sums[kind, step, rows, :] = value.astype(jnp.bfloat16)
            return carry

        lax.fori_loop(0, 8, add, 0)
        for d in (2, 1, 3):
            two_copy(kind, step, d).start()

    def last(kind, step):
        f = first_axis(kind, step)
        mine = two_pos(kind, f)
        wait_for(sums_in.at[kind, step, pl.ds(0, 96), :], two_sem.at[kind, step])
        if kind == 0:
            value = sums[kind, step, quarter(mine), :].astype(jnp.float32)
            for d in range(1, 4):
                value = value + sums_in[kind, step, quarter(mine + d), :].astype(jnp.float32)
            out[0, pl.ds(pl.multiple_of(step * WA, WA), WA), :] = value
        else:
            for e in range(2):
                zl = lax.rem(low + e, 2)

                def rows(pos):
                    return pl.ds(pl.multiple_of(lax.rem(pos, 4) * 32 + zl * WB, WB), WB)

                value = sums[kind, step, rows(mine), :].astype(jnp.float32)
                for d in range(1, 4):
                    value = value + sums_in[kind, step, rows(mine + d), :].astype(jnp.float32)
                if e == 0:
                    out[0, row_b(low, step), :] = value
                else:
                    swap[step] = value.astype(jnp.bfloat16)
            swap_copy(step).start()

    def body(step, carry):
        @pl.when(step + AHEAD < STEPS)
        def _():
            for kind in range(2):
                send_slab(kind, step + AHEAD)

        for kind in (1, 0):
            produce(kind, step)

            @pl.when(step >= LAG0)
            def _():
                forward(kind, step - LAG0)

            @pl.when(step >= LAG1)
            def _():
                middle(kind, step - LAG1)

        @pl.when(step >= LAG2)
        def _():
            for kind in range(2):
                last(kind, step - LAG2)

        return carry

    lax.fori_loop(0, STEPS, body, 0)
    def finish(step, carry):
        @pl.when(step < STEPS + LAG0)
        def _():
            for kind in (1, 0):
                forward(kind, step - LAG0)

        @pl.when(step < STEPS + LAG1)
        def _():
            for kind in (1, 0):
                middle(kind, step - LAG1)

        for kind in (1, 0):
            last(kind, step - LAG2)
        return carry

    lax.fori_loop(STEPS, STEPS + LAG2, finish, 0)

    for kind in range(2):
        slab = slab_a if kind == 0 else slab_b
        wait_for(feats.at[kind, :, pl.ds(0, 896), :], feat_out.at[kind])
        wait_for(slab.at[:, :, :, :, pl.ds(0, 896)], slab_out.at[kind])
    wait_for(relay, one_out.at[0])
    wait_for(part_in, one_out.at[1])
    wait_for(sums_in.at[:, :, pl.ds(0, 96), :], two_out.at[0])
    wait_for(swap, swap_out.at[0])
    wait_for(swap_in, swap_sem.at[0])
    half = pl.ds(pl.multiple_of(BASE_B + (1 - low) * (STEPS * WB), WB), STEPS * WB)
    out[0, half, :] = swap_in[...].reshape(STEPS * WB, 512).astype(jnp.float32)


def per_device(weight, activation, points):
    hbm = pl.BlockSpec(memory_space=pltpu.HBM)
    dma = pltpu.SemaphoreType.DMA
    return pl.pallas_call(
        kernel,
        out_shape=jax.ShapeDtypeStruct((1, 512, 512), jnp.float32),
        in_specs=[hbm, hbm, hbm],
        out_specs=pl.BlockSpec(memory_space=pltpu.VMEM),
        scratch_shapes=[
            pltpu.VMEM((STEPS, 4, 2, WA, 1024), jnp.bfloat16),
            pltpu.VMEM((STEPS, 4, 4, WB, 1024), jnp.bfloat16),
            pltpu.VMEM((2, 2, 1024, 512), jnp.bfloat16),
            pltpu.VMEM((2, 4, 64, 512), jnp.float32),
            pltpu.VMEM((2, STEPS, 4, 128, 512), jnp.bfloat16),
            pltpu.VMEM((2, STEPS, 2, 64, 512), jnp.bfloat16),
            pltpu.VMEM((2, STEPS, 2, 128, 512), jnp.bfloat16),
            pltpu.VMEM((2, STEPS, 128, 512), jnp.bfloat16),
            pltpu.VMEM((2, STEPS, 128, 512), jnp.bfloat16),
            pltpu.VMEM((STEPS, WB, 512), jnp.bfloat16),
            pltpu.VMEM((STEPS, WB, 512), jnp.bfloat16),
            pltpu.SMEM((8,), jnp.int32),
            dma((2, STEPS)), dma((2,)), dma((2, 3)), dma((2,)), dma((2,)),
            dma((2, STEPS, 2)), dma((2,)), dma((2, STEPS)), dma((1,)), dma((1,)), dma((1,)), dma((3,)),
        ],
        compiler_params=pltpu.CompilerParams(
            collective_id=0, has_side_effects=True, vmem_limit_bytes=52 * 2**20),
        name="coded_share",
    )(weight.reshape(4, 2, 4, 2, 512, 128), activation, points)


def solution(mesh):
    placed = (P(None, None, ("grp", "mem")), P(None, ("grp", "mem"), None), P())
    return jax.shard_map(
        per_device, mesh=mesh, in_specs=placed, out_specs=P("grp", "mem", None), check_vma=False
    )
```
